256 devices in a mesh: node: 8 (over x, core), chip: 32 (over y, z).
Axes of the slice: x: 4, y: 4, z: 8, core: 2. Of those that a mesh axis runs over, the one named last changes fastest.
Arguments:
- table: float32 [2, 1048576, 128], P(None, ('node', 'chip')), may hold values from -1.5 to 1.5
- unique_ids: int32 [256, 2, 4096], P(('node', 'chip')), may hold values from 0 to 4095, as said below
- counts: int32 [256, 2, 256], P(('node', 'chip')), may hold values from 12 to 16, as said below
- inverse: int32 [131072, 2, 40], P(('node', 'chip')), may hold values from 0 to 4095, as said below
- lengths: int32 [131072, 2], P(('node', 'chip')), may hold values from 1 to 40
Outputs:
- pooled: float32 [131072, 2, 128], P(('node', 'chip'))
The draws below stay inside these ranges and needn't reach their ends.
Inputs may be any that keep to these rules, and one draw needn't show every extreme that they name: `counts`: for every device and table some owner receives exactly 16, and for every table some owner receives 16 from every device. `unique_ids`: entries u with offsets[o] <= u < offsets[o] + counts[o] are distinct row numbers of owner o; entries past the total are unused. `inverse`: every entry is below the sum of counts of its device and table.
All inputs are finite; a program needn't handle non-finite values.
Results may differ from the reference program's by a relative error of at most 0.0003.
Values sent between devices are 32-bit elements; how exact they have to be, the bound alone decides.
A program may use at most 64 MiB of HBM per device.

```python
import jax
import jax.numpy as jnp
from jax import lax

WIDTH = 128
TABLES = 2
ROWS_DEV = 4096
CAP = 16
SAMP_DEV = 512
POOL = 40
ROWS = 1048576
SAMPLES = 131072
UNIQ = 4096
DEVICES = 256


def shared_counts(key):
    base_key = jax.random.fold_in(key, 11)
    hot_key = jax.random.fold_in(key, 12)
    pick_key = jax.random.fold_in(key, 13)
    base = jax.random.randint(base_key, (DEVICES, TABLES, DEVICES), CAP - CAP // 4, CAP + 1)
    hot = jax.random.randint(hot_key, (TABLES, 4), 0, DEVICES)
    owners = jnp.arange(DEVICES, dtype=jnp.int32)
    is_hot = jnp.any(owners[None, :, None] == hot[:, None, :], axis=2)
    picked = jax.random.randint(pick_key, (DEVICES, TABLES, 1), 0, DEVICES)
    full = is_hot[None, :, :] | (owners[None, None, :] == picked)
    return jnp.where(full, CAP, base).astype(jnp.int32)


def draw_counts(key, part):
    return shared_counts(key)


def draw_unique_ids(key, part):
    counts = shared_counts(key)
    inclusive = jnp.cumsum(counts, axis=2)
    offsets = inclusive - counts
    slots = jnp.arange(UNIQ, dtype=jnp.int32)
    owner = jax.vmap(jax.vmap(lambda inc: jnp.minimum(jnp.searchsorted(inc, slots, side='right'), DEVICES - 1)))(inclusive)
    start = jnp.take_along_axis(offsets, owner, axis=2)
    within = slots[None, None, :] - start
    base = jax.random.randint(jax.random.fold_in(key, 21), (DEVICES, TABLES, DEVICES), 0, ROWS_DEV)
    owner_base = jnp.take_along_axis(base, owner, axis=2)
    ids = (owner_base + within) % ROWS_DEV
    filler = jax.random.randint(jax.random.fold_in(key, 22), (DEVICES, TABLES, UNIQ), 0, ROWS_DEV)
    total = inclusive[:, :, -1:]
    return jnp.where(slots[None, None, :] < total, ids, filler).astype(jnp.int32)


def draw_inverse(key, part):
    counts = shared_counts(key)
    total = jnp.sum(counts, axis=2)
    bound = jnp.repeat(total, SAMP_DEV, axis=0)
    return jax.random.randint(jax.random.fold_in(key, 31), (SAMPLES, TABLES, POOL), 0, bound[:, :, None]).astype(jnp.int32)


def touch_ends(entries, key, smallest, high):
    shape = entries.shape
    place = [jax.random.randint(jax.random.fold_in(key, axis), (), 0, shape[axis]) for axis in range(len(shape))]
    entries = entries.at[tuple(place)].set(smallest)
    longest = shape.index(max(shape))
    place[longest] = (place[longest] + 1) % shape[longest]
    return entries.at[tuple(place)].set(high)


def steps_of(key, shape, cuts, least, high):
    loudness = 1.0
    for axis_at, parts in cuts:
        draws = jax.random.uniform(jax.random.fold_in(jax.random.fold_in(key, 6), axis_at), (parts,), jnp.float32, least / len(cuts), high / len(cuts))
        loudness = loudness * jnp.repeat(jnp.exp(draws), shape[axis_at] // parts).reshape((-1,) + (1,) * (len(shape) - 1 - axis_at))
    return loudness


def gaussian(own_key, shape, scale, limit, split=(), kind=jnp.bfloat16):
    values = jax.random.normal(own_key, shape, jnp.float32) * scale
    if len(split) > 0:
        values = steps_of(own_key, shape, split, -0.22, 0.18) * values
    return jnp.clip(values, min=-limit, max=limit).astype(kind)


def setup_inputs(seed: int = 0) -> dict:
    arg_keys = jax.random.split(jax.random.key(seed), 6)
    table = gaussian(arg_keys[0], (TABLES, ROWS, WIDTH), 0.25, 1.5, ((1, 256),), jnp.float32)
    unique_ids = draw_unique_ids(jax.random.fold_in(arg_keys[5], 71), 0)
    counts = draw_counts(jax.random.fold_in(arg_keys[5], 71), 0)
    inverse = draw_inverse(jax.random.fold_in(arg_keys[5], 71), 0)
    lengths = touch_ends(jax.random.randint(arg_keys[4], (SAMPLES, TABLES), 1, POOL + 1), jax.random.fold_in(arg_keys[4], 1), 1, POOL).astype(jnp.int32)
    return dict(table=table, unique_ids=unique_ids, counts=counts, inverse=inverse, lengths=lengths)


def one_device(d, table, unique_ids, counts, inverse, lengths):
    ids = unique_ids[d]
    count = counts[d]
    inv = lax.dynamic_slice_in_dim(inverse, (d * SAMP_DEV).astype(jnp.int32), SAMP_DEV, 0)
    lens = lax.dynamic_slice_in_dim(lengths, (d * SAMP_DEV).astype(jnp.int32), SAMP_DEV, 0)
    positions = jnp.arange(POOL, dtype=jnp.int32)
    outs = []
    for t in range(TABLES):
        inclusive = jnp.cumsum(count[t]).astype(jnp.int32)
        index = inv[:, t, :]
        owner = jnp.minimum(jnp.searchsorted(inclusive, index, side="right").astype(jnp.int32), DEVICES - 1)
        rows = owner * ROWS_DEV + ids[t][index]
        vectors = table[t][rows]
        mask = positions[None, :] < lens[:, t][:, None]
        outs.append(jnp.sum(jnp.where(mask[:, :, None], vectors, jnp.zeros((), jnp.float32)), axis=1))
    return jnp.stack(outs, axis=1)


def reference(table, unique_ids, counts, inverse, lengths):
    result = lax.map(lambda d: one_device(d, table, unique_ids, counts, inverse, lengths), jnp.arange(DEVICES, dtype=jnp.int32))
    return result.reshape(SAMPLES, TABLES, WIDTH)
```

```python
import functools

import jax
import jax.numpy as jnp
from jax import lax
from jax.experimental import pallas as pl
from jax.experimental.pallas import tpu as pltpu
from jax.sharding import PartitionSpec as P

MESH = pl.DeviceIdType.MESH
NZ = 8
CORES = 2
FIELDS = 4
BITS = 8

ROUTES = (
    (4, None, None, None),
    (3, 1, 2, 1),
    (5, -1, 1, 1),
    (2, 0, 2, 0),
    (6, 0, 1, 0),
    (1, 1, 0, 0),
    (7, -1, 0, 2),
    (0, 0, 0, 1),
)


def kernel(
    dims,
    counts,
    ids,
    inv,
    lens,
    table_hbm,
    out,
    table,
    start,
    msg,
    idbuf,
    idnum,
    code,
    code_in,
    group_of,
    unit_of,
    weight,
    send,
    recv,
    acc,
    part,
    ready,
    table_sem,
    id_send,
    id_recv,
    num_sem,
    code_send,
    code_recv,
    row_send,
    row_recv,
    part_send,
    part_recv,
):
    nx, ny, cap, rows_dev = dims
    q_all = nx * CORES * ny
    owners = q_all * NZ
    tables, depth, samples = inv.shape
    slots = q_all * cap
    words = slots // FIELDS
    node, chip = lax.axis_index("node"), lax.axis_index("chip")
    n_node, n_chip = nx * CORES, ny * NZ
    x, c, y, z = node // CORES, node % CORES, chip // NZ, chip % NZ
    mine = node * ny + y

    def place(dx, dy, dc, dz):
        return (
            ((x + dx) % nx) * CORES + (c + dc) % CORES,
            ((y + dy) % ny) * NZ + (z + dz) % NZ,
        )

    def step_of(i):
        return (i // CORES) % nx, i // n_node, i % CORES

    barrier = pltpu.get_barrier_semaphore()
    row = [(node, (chip + i) % n_chip) for i in range(1, n_chip)]
    column = [((node + i) % n_node, chip) for i in range(1, n_node)]
    for peer in row + column:
        pl.semaphore_signal(barrier, inc=1, device_id=peer, device_id_type=MESH)
    fetch = pltpu.make_async_copy(table_hbm, table, table_sem)
    fetch.start()

    def add_up(o, sums):
        new = []
        for t in range(tables):
            start[t, o] = sums[t]
            new.append(sums[t] + counts[t, o])
        return tuple(new)

    lax.fori_loop(0, owners, add_up, (jnp.int32(0),) * tables)

    lane = lax.broadcasted_iota(jnp.int32, (1, 128), 1)
    last = ids.shape[0] - 1

    def write_message(k, _):
        dx, dy, dc = step_of(k % q_all)
        dz = k // q_all
        on, oc = place(-dx, -dy, -dc, -dz)
        o = on * n_chip + oc
        pieces = []
        for t in range(tables):
            at = start[t, o]
            r = jnp.minimum(at >> 7, last)
            l = at & 127
            a = ids[r, pl.ds(t, 1), :]
            b = ids[jnp.minimum(r + 1, last), pl.ds(t, 1), :]
            both = jnp.where(lane < l, b, a)
            pieces.append(pltpu.roll(both, (cap * t - l) & 127, 1))
        line = jnp.where(lane < cap, pieces[0], pieces[1])
        msg[k] = jnp.clip(line, 0, rows_dev - 1)
        return 0

    lax.fori_loop(0, owners, write_message, 0)

    pl.semaphore_wait(barrier, n_chip + n_node - 2)
    for peer in column:
        pl.semaphore_signal(ready, inc=1, device_id=peer, device_id_type=MESH)
    pl.semaphore_wait(ready, n_node - 1)

    def send_ids(k, delta):
        dx, dy, dc = step_of(k % q_all)
        pltpu.make_async_remote_copy(
            msg.at[k],
            idbuf.at[k],
            id_send,
            id_recv.at[delta],
            device_id=place(-dx, -dy, -dc, -delta),
            device_id_type=MESH,
        ).start()

    for delta, _, _, _ in ROUTES:

        def one(i, _, delta=delta):
            send_ids(delta * q_all + i, delta)
            return 0

        lax.fori_loop(1 if delta == 0 else 0, q_all, one, 0)

    position = lax.broadcasted_iota(jnp.int32, (depth, samples), 0)
    for t in range(tables):
        index = inv[t]

        def shift(o, slot, t=t, index=index):
            n = counts[t, o]
            return slot + jnp.where(index >= start[t, o] + n, cap - n, 0)

        slot = lax.fori_loop(0, owners - 1, shift, index, unroll=5)
        plane = (slot // cap) % NZ
        value = plane * slots + (slot // (cap * NZ)) * cap + slot % cap
        code[t] = jnp.where(position < lens[t], value, -1)
    code_copies = []
    for side, dz in ((0, 2), (1, -2)):
        copy = pltpu.make_async_remote_copy(
            code,
            code_in[side],
            code_send.at[side],
            code_recv.at[side],
            device_id=place(0, 0, 0, dz),
            device_id_type=MESH,
        )
        copy.start()
        code_copies.append(copy)

    def split_codes(source, g):
        for t in range(tables):
            v = source[t]
            live = v >= 0
            inside = v % slots
            group_of[g, t] = jnp.where(live, (v // slots) * words + inside % words, -1)
            unit_of[g, t] = jnp.where(live, 1 << (BITS * (inside // words)), 0)

    lanes = min(128, samples)
    rows_at = lax.broadcasted_iota(jnp.int32, (words, lanes), 0)

    def count(w, g, t, plane):
        wanted = rows_at + plane * words

        def tile(i, _):
            at = pl.multiple_of(i * lanes, lanes)

            def step(n, total):
                rows = pl.ds(pl.multiple_of(n * 8, 8), 8)
                groups = group_of.at[g, t, rows, pl.ds(at, lanes)]
                units = unit_of.at[g, t, rows, pl.ds(at, lanes)]
                for p in range(8):
                    hit = groups[pl.ds(p, 1), :] == wanted
                    total = total + jnp.where(hit, units[pl.ds(p, 1), :], 0)
                return total

            total = lax.fori_loop(0, depth // 8, step, jnp.zeros((words, lanes), jnp.int32))
            for f in range(FIELDS):
                part_count = (total >> (BITS * f)) & ((1 << BITS) - 1)
                weight[w, pl.ds(f * words, words), pl.ds(at, lanes)] = part_count.astype(
                    jnp.float32
                ).astype(jnp.bfloat16)
            return 0

        lax.fori_loop(0, samples // lanes, tile, 0)

    works = [[], [], []]
    n_work = 0
    for g, planes in ((0, (-1, 0, 1)), (1, (0, 1, 2)), (2, (0, -1, -2))):
        for b, dz in enumerate(planes):
            for t in range(tables):
                if g and b == 2 and t != g - 1:
                    continue
                works[g].append((b, t, n_work, dz))
                n_work += 1

    split_codes(code, 0)
    for b, t, w, dz in works[0]:
        count(w, 0, t, (z + dz) % NZ)

    def ids_ready(delta):
        rows = pl.ds(delta * q_all, q_all) if delta else pl.ds(1, q_all - 1)
        got = idbuf.at[rows]
        pltpu.make_async_copy(got, got, id_recv.at[delta]).wait()
        copy = pltpu.make_async_copy(got, idnum.at[rows], num_sem.at[delta])
        copy.start()
        return copy

    def collect(k):
        for t in range(tables):
            for s in range(cap):
                r = idnum[k, 0, t * cap + s]
                send[k, t, pl.ds(s, 1), :] = table[t * rows_dev + r]

    def send_rows(k, i, delta, dz, g, b):
        dx, dy, dc = step_of(i)

        def go(source, target, sem, dz):
            pltpu.make_async_remote_copy(
                source,
                target,
                row_send,
                row_recv.at[sem],
                device_id=place(dx, dy, dc, dz),
                device_id_type=MESH,
            ).start()

        if g is None:
            go(send.at[k, 0], recv[5].at[mine], 5, -2)
            go(send.at[k, 1], recv[8].at[mine], 8, 2)
        else:
            go(send.at[k], recv[3 * g + b].at[mine], 3 * g + b, dz)

    own_ids = pltpu.make_async_copy(
        msg.at[pl.ds(0, 1)], idnum.at[pl.ds(0, 1)], num_sem.at[NZ]
    )
    own_ids.start()
    copies = [ids_ready(ROUTES[0][0])]
    copies += [ids_ready(route[0]) for route in ROUTES[1:]]
    fetch.wait()
    own_ids.wait()
    for copy in copies:
        copy.wait()
    for delta, dz, g, b in ROUTES:
        stay = dz == 0
        if stay:
            k0 = delta * q_all
            collect(k0)
            pltpu.make_async_copy(
                send.at[k0], recv[3 * g + b].at[mine], row_recv.at[3 * g + b]
            ).start()

        def serve(i, _, delta=delta, dz=dz, g=g, b=b):
            k = delta * q_all + i
            collect(k)
            send_rows(k, i, delta, dz, g, b)
            return 0

        lax.fori_loop(1 if stay else 0, q_all, serve, 0)

    def rows_ready(g, b):
        got = recv[3 * g + b]
        pltpu.make_async_copy(got, got, row_recv.at[3 * g + b]).wait()

    def pool(g, b, t, w, first):
        block = recv[3 * g + b]
        rows = block[...] if g and b == 2 else block[:, t]
        rows = rows.reshape(slots, 128).T
        high = rows.astype(jnp.bfloat16)
        low = (rows - high.astype(jnp.float32)).astype(jnp.bfloat16)
        both = jnp.dot(
            jnp.concatenate([high, low], axis=0), weight[w], preferred_element_type=jnp.float32
        )
        new = both[:128] + both[128:]
        total = acc[tables * g + t]
        total[...] = new if first else total[...] + new

    part_copies = []
    for g in (1, 2):
        code_copies[g - 1].wait_recv()
        split_codes(code_in[g - 1], g)
        for b, t, w, dz in works[g]:
            count(w, g, t, (z + dz) % NZ)
    for g in (1, 2):
        for b in range(3):
            rows_ready(g, b)
        for t in (2 - g, g - 1):
            todo = [work for work in works[g] if work[1] == t]
            for n, (b, _, w, _) in enumerate(todo):
                pool(g, b, t, w, n == 0)
            copy = pltpu.make_async_remote_copy(
                acc[tables * g + t],
                part[tables * (g - 1) + t],
                part_send.at[g - 1, t],
                part_recv.at[g - 1, t],
                device_id=place(0, 0, 0, -2 if g == 1 else 2),
                device_id_type=MESH,
            )
            copy.start()
            part_copies.append((t, copy))

    done = set()
    for b in (1, 0, 2):
        rows_ready(0, b)
        for bb, t, w, _ in works[0]:
            if bb == b:
                pool(0, b, t, w, t not in done)
                done.add(t)
    for t in range(tables):
        for tt, copy in part_copies:
            if tt == t:
                copy.wait_recv()
        out[t] = (acc[t][...] + (part[t][...] + part[tables + t][...])).T

    for copy in code_copies:
        copy.wait_send()
    for _, copy in part_copies:
        copy.wait_send()
    pltpu.make_async_copy(msg.at[pl.ds(1, owners - 1)], msg.at[pl.ds(1, owners - 1)], id_send).wait()
    sent = send.at[pl.ds(0, owners - 3)]
    pltpu.make_async_copy(sent, sent, row_send).wait()


def local(sizes, table, unique_ids, counts, inverse, lengths):
    nx, ny = sizes
    tables, rows_dev, width = table.shape
    owners = counts.shape[2]
    uniq = unique_ids.shape[2]
    cap = uniq // owners
    samples, _, depth = inverse.shape
    q_all = nx * CORES * ny
    slots = q_all * cap
    dims = (nx, ny, cap, rows_dev)
    vmem = pl.BlockSpec(memory_space=pltpu.VMEM)
    block = pltpu.VMEM((q_all, tables, cap, width), jnp.float32)
    far = pltpu.VMEM((q_all, cap, width), jnp.float32)
    out = pl.pallas_call(
        functools.partial(kernel, dims),
        out_shape=jax.ShapeDtypeStruct((tables, samples, width), jnp.float32),
        in_specs=[
            pl.BlockSpec(memory_space=pltpu.SMEM),
            vmem,
            vmem,
            vmem,
            pl.BlockSpec(memory_space=pl.ANY),
        ],
        out_specs=vmem,
        scratch_shapes=[
            pltpu.VMEM((tables * rows_dev, 1, width), jnp.float32),
            pltpu.SMEM((tables, owners), jnp.int32),
            pltpu.VMEM((owners, 1, 128), jnp.int32),
            pltpu.VMEM((owners, 1, 128), jnp.int32),
            pltpu.SMEM((owners, 1, 128), jnp.int32),
            pltpu.VMEM((tables, depth, samples), jnp.int32),
            [pltpu.VMEM((tables, depth, samples), jnp.int32)] * 2,
            pltpu.VMEM((3, tables, depth, samples), jnp.int32),
            pltpu.VMEM((3, tables, depth, samples), jnp.int32),
            pltpu.VMEM((16, slots, samples), jnp.bfloat16),
            pltpu.VMEM((owners, tables, cap, width), jnp.float32),
            [block, block, block, block, block, far, block, block, far],
            [pltpu.VMEM((width, samples), jnp.float32)] * (3 * tables),
            [pltpu.VMEM((width, samples), jnp.float32)] * (2 * tables),
            pltpu.SemaphoreType.REGULAR,
            pltpu.SemaphoreType.DMA,
            pltpu.SemaphoreType.DMA,
            pltpu.SemaphoreType.DMA((NZ,)),
            pltpu.SemaphoreType.DMA((NZ + 1,)),
            pltpu.SemaphoreType.DMA((2,)),
            pltpu.SemaphoreType.DMA((2,)),
            pltpu.SemaphoreType.DMA,
            pltpu.SemaphoreType.DMA((9,)),
            pltpu.SemaphoreType.DMA((2, 2)),
            pltpu.SemaphoreType.DMA((2, 2)),
        ],
        compiler_params=pltpu.CompilerParams(
            collective_id=0, has_side_effects=True, vmem_limit_bytes=56 << 20
        ),
        name="bags",
    )(
        counts[0],
        unique_ids.reshape(tables, uniq // 128, 128).transpose(1, 0, 2),
        inverse.transpose(1, 2, 0),
        lengths.T.reshape(tables, 1, samples),
        table.reshape(tables * rows_dev, 1, width),
    )
    return out.transpose(1, 0, 2)


def solution(mesh):
    sizes = (mesh.shape["node"] // CORES, mesh.shape["chip"] // NZ)
    return jax.shard_map(
        functools.partial(local, sizes),
        mesh=mesh,
        in_specs=(
            P(None, ("node", "chip"), None),
            P(("node", "chip"), None, None),
            P(("node", "chip"), None, None),
            P(("node", "chip"), None, None),
            P(("node", "chip"), None),
        ),
        out_specs=P(("node", "chip"), None, None),
        check_vma=False,
    )
```

```python
import functools

import jax
import jax.numpy as jnp
from jax import lax
from jax.experimental import pallas as pl
from jax.experimental.pallas import tpu as pltpu
from jax.sharding import PartitionSpec as P

MESH = pl.DeviceIdType.MESH
NZ = 8
CORES = 2
FIELDS = 4
BITS = 8

FAR = (
    ((4, -2, 1, 2), (5, -1, 1, 1), (3, 1, 2, 1), (6, 0, 1, 0), (2, 0, 2, 0)),
    ((4, 2, 2, 2), (3, 1, 2, 1), (5, -1, 1, 1), (2, 0, 2, 0), (6, 0, 1, 0)),
)
NEAR = ((1, 1, 0, 0), (7, -1, 0, 2), (0, 0, 0, 1))
ID_ORDER = (4, 5, 3, 6, 2, 1, 7, 0)


def near_slot(b):
    return b


def far_slot(t, g, b):
    at = [(route[2], route[3]) for route in FAR[t]].index((g, b))
    return len(NEAR) + t * len(FAR[0]) + at


def kernel(
    dims,
    counts,
    ids,
    inv,
    lens,
    table_hbm,
    out,
    table,
    start,
    msg,
    idbuf,
    idnum,
    code,
    code_in,
    group_of,
    unit_of,
    weight,
    send,
    recv,
    acc,
    part,
    ready,
    table_sem,
    id_send,
    id_recv,
    num_sem,
    code_send,
    code_recv,
    row_send,
    row_recv,
    part_send,
    part_recv,
):
    nx, ny, cap, rows_dev = dims
    q_all = nx * CORES * ny
    owners = q_all * NZ
    tables, depth, samples = inv.shape
    slots = q_all * cap
    words = slots // FIELDS
    node, chip = lax.axis_index("node"), lax.axis_index("chip")
    n_node, n_chip = nx * CORES, ny * NZ
    x, c, y, z = node // CORES, node % CORES, chip // NZ, chip % NZ
    mine = node * ny + y

    steps = [(dx, dc) for dx in range(nx) for dc in range(CORES)]
    node_to = [lax.rem(x + dx, nx) * CORES + lax.rem(c + dc, CORES) for dx, dc in steps]
    node_from = [
        lax.rem(x + nx - dx, nx) * CORES + lax.rem(c + CORES - dc, CORES) for dx, dc in steps
    ]

    def chip_at(dy, dz):
        return lax.rem(y + ny + dy, ny) * NZ + lax.rem(z + NZ + dz, NZ)

    def above(dz):
        return node, chip_at(0, dz)

    barrier = pltpu.get_barrier_semaphore()
    row = [(node, (chip + i) % n_chip) for i in range(1, n_chip)]
    column = [((node + i) % n_node, chip) for i in range(1, n_node)]
    for peer in row + column:
        pl.semaphore_signal(barrier, inc=1, device_id=peer, device_id_type=MESH)
    fetch = pltpu.make_async_copy(table_hbm, table, table_sem)
    fetch.start()

    lane = lax.broadcasted_iota(jnp.int32, (1, 128), 1)
    last = ids.shape[0] - 1

    def write_messages(n, sums):
        sums = list(sums)
        for u in range(8):
            o = n * 8 + u
            pieces = []
            for t in range(tables):
                at = sums[t]
                start[t, o] = at
                sums[t] = at + counts[t, o]
                r = jnp.minimum(at >> 7, last)
                l = at & 127
                a = ids[r, pl.ds(t, 1), :]
                b = ids[jnp.minimum(r + 1, last), pl.ds(t, 1), :]
                both = jnp.where(lane < l, b, a)
                pieces.append(pltpu.roll(both, (cap * t - l) & 127, 1))
            line = jnp.where(lane < cap, pieces[0], pieces[1])
            msg[o] = jnp.clip(line, 0, rows_dev - 1)
        return tuple(sums)

    lax.fori_loop(0, owners // 8, write_messages, (jnp.int32(0),) * tables)

    pl.semaphore_wait(barrier, n_chip + n_node - 2)
    for peer in column:
        pl.semaphore_signal(ready, inc=1, device_id=peer, device_id_type=MESH)
    pl.semaphore_wait(ready, n_node - 1)

    def send_ids(delta, dy, j):
        to = (node_from[j], chip_at(-dy, -delta))
        pltpu.make_async_remote_copy(
            msg.at[to[0] * n_chip + to[1]],
            idbuf.at[delta * q_all + dy * n_node + j],
            id_send,
            id_recv.at[delta],
            device_id=to,
            device_id_type=MESH,
        ).start()

    for delta in ID_ORDER:

        def one(dy, _, delta=delta):
            for j in range(n_node):
                if delta == 0 and j == 0:

                    @pl.when(dy > 0)
                    def _():
                        send_ids(delta, dy, j)
                else:
                    send_ids(delta, dy, j)
            return 0

        lax.fori_loop(0, ny, one, 0)

    position = lax.broadcasted_iota(jnp.int32, (depth, samples), 0)
    for t in range(tables):
        index = inv[t]

        def shift(o, slot, t=t, index=index):
            n = counts[t, o]
            return slot + jnp.where(index >= start[t, o] + n, cap - n, 0)

        slot = lax.fori_loop(0, owners - 1, shift, index, unroll=5)
        plane = (slot // cap) % NZ
        value = plane * slots + (slot // (cap * NZ)) * cap + slot % cap
        code[t] = jnp.where(position < lens[pl.ds(t, 1), :], value, -1)
    code_copies = []
    for side, dz in ((0, 2), (1, -2)):
        copy = pltpu.make_async_remote_copy(
            code,
            code_in[side],
            code_send.at[side],
            code_recv.at[side],
            device_id=above(dz),
            device_id_type=MESH,
        )
        copy.start()
        code_copies.append(copy)

    def split_codes(source, g):
        for t in range(tables):
            v = source[t]
            live = v >= 0
            inside = v % slots
            group_of[g, t] = jnp.where(live, (v // slots) * words + inside % words, -1)
            unit_of[g, t] = jnp.where(live, 1 << (BITS * (inside // words)), 0)

    lanes = min(128, samples)
    rows_at = lax.broadcasted_iota(jnp.int32, (words, lanes), 0)

    def count(w, g, t, plane):
        wanted = rows_at + plane * words

        def tile(i, _):
            at = pl.multiple_of(i * lanes, lanes)

            def step(n, total):
                rows = pl.ds(pl.multiple_of(n * 8, 8), 8)
                groups = group_of.at[g, t, rows, pl.ds(at, lanes)]
                units = unit_of.at[g, t, rows, pl.ds(at, lanes)]
                for p in range(8):
                    hit = groups[pl.ds(p, 1), :] == wanted
                    total = total + jnp.where(hit, units[pl.ds(p, 1), :], 0)
                return total

            total = lax.fori_loop(0, depth // 8, step, jnp.zeros((words, lanes), jnp.int32))
            for f in range(FIELDS):
                part_count = (total >> (BITS * f)) & ((1 << BITS) - 1)
                weight[w, pl.ds(f * words, words), pl.ds(at, lanes)] = part_count.astype(
                    jnp.float32
                ).astype(jnp.bfloat16)
            return 0

        lax.fori_loop(0, samples // lanes, tile, 0)

    works = []
    for b in range(3):
        works += [(near_slot(b), 0, t, 2 * b + t, b - 1) for t in range(tables)]
    for t in range(tables):
        for _, _, g, b in FAR[t]:
            works.append((far_slot(t, g, b), g, t, len(works), b if g == 1 else -b))

    def count_all(g, t):
        for _, gg, tt, w, dz in works:
            if (gg, tt) == (g, t):
                count(w, g, t, lax.rem(z + NZ + dz, NZ))

    def ids_ready(delta):
        rows = pl.ds(delta * q_all, q_all) if delta else pl.ds(1, q_all - 1)
        got = idbuf.at[rows]
        pltpu.make_async_copy(got, got, id_recv.at[delta]).wait()
        copy = pltpu.make_async_copy(got, idnum.at[rows], num_sem.at[delta])
        copy.start()
        return copy

    def collect(k, t):
        for s in range(cap):
            r = idnum[k, 0, t * cap + s]
            send[k, t, pl.ds(s, 1), :] = table[t * rows_dev + r]

    def serve(delta, dz, slot, t):
        def piece(k):
            return send.at[k] if t is None else send.at[k, t]

        def send_rows(k, dy, j):
            pltpu.make_async_remote_copy(
                piece(k),
                recv[slot].at[mine],
                row_send,
                row_recv.at[slot],
                device_id=(node_to[j], chip_at(dy, dz)),
                device_id_type=MESH,
            ).start()

        def line(dy, _):
            for j in range(n_node):
                k = delta * q_all + dy * n_node + j
                for tt in range(tables):
                    if t is None or t == tt:
                        collect(k, tt)
                if dz == 0 and j == 0:

                    @pl.when(dy > 0)
                    def _():
                        send_rows(k, dy, j)

                    @pl.when(dy == 0)
                    def _():
                        pltpu.make_async_copy(
                            piece(k), recv[slot].at[mine], row_recv.at[slot]
                        ).start()
                else:
                    send_rows(k, dy, j)
            return 0

        lax.fori_loop(0, ny, line, 0)

    def serve_far(t):
        for delta, dz, g, b in FAR[t]:
            serve(delta, dz, far_slot(t, g, b), t)

    own_ids = pltpu.make_async_copy(
        msg.at[pl.ds(node * n_chip + chip, 1)], idnum.at[pl.ds(0, 1)], num_sem.at[NZ]
    )
    own_ids.start()
    copies = [ids_ready(delta) for delta in ID_ORDER]
    fetch.wait()
    own_ids.wait()
    for copy in copies:
        copy.wait()

    def rows_ready(slot):
        got = recv[slot]
        pltpu.make_async_copy(got, got, row_recv.at[slot]).wait()

    def pool(slot, g, t, w, first):
        rows = recv[slot][:, t] if g == 0 else recv[slot][...]
        rows = rows.reshape(slots, 128).T
        high = rows.astype(jnp.bfloat16)
        low = (rows - high.astype(jnp.float32)).astype(jnp.bfloat16)
        both = jnp.dot(
            jnp.concatenate([high, low], axis=0), weight[w], preferred_element_type=jnp.float32
        )
        new = both[:128] + both[128:]
        total = acc[tables * g + t]
        total[...] = new if first else total[...] + new

    part_copies = []

    def pool_far(t):
        for g in ((1, 2), (2, 1))[t]:
            mine_now = [work for work in works if work[1:3] == (g, t)]
            for n, (slot, _, _, w, _) in enumerate(mine_now):
                rows_ready(slot)
                pool(slot, g, t, w, n == 0)
            copy = pltpu.make_async_remote_copy(
                acc[tables * g + t],
                part[tables * (g - 1) + t],
                part_send.at[g - 1, t],
                part_recv.at[g - 1, t],
                device_id=above(-2 if g == 1 else 2),
                device_id_type=MESH,
            )
            copy.start()
            part_copies.append((t, copy))

    serve_far(0)
    for g in (1, 2):
        code_copies[g - 1].wait_recv()
        split_codes(code_in[g - 1], g)
        count_all(g, 0)
    serve_far(1)
    for g in (1, 2):
        count_all(g, 1)
    pool_far(0)
    for delta, dz, _, b in NEAR:
        serve(delta, dz, near_slot(b), None)
    split_codes(code, 0)
    for t in range(tables):
        count_all(0, t)
    pool_far(1)

    for n, b in enumerate((1, 0, 2)):
        rows_ready(near_slot(b))
        for slot, g, t, w, _ in works:
            if g == 0 and slot == near_slot(b):
                pool(slot, g, t, w, n == 0)
    for t in range(tables):
        for tt, copy in part_copies:
            if tt == t:
                copy.wait_recv()
        out[pl.ds(t, samples, stride=tables), :] = (
            acc[t][...] + (part[t][...] + part[tables + t][...])
        ).T

    for copy in code_copies:
        copy.wait_send()
    for _, copy in part_copies:
        copy.wait_send()
    pltpu.make_async_copy(msg.at[pl.ds(1, owners - 1)], msg.at[pl.ds(1, owners - 1)], id_send).wait()
    sent = send.at[pl.ds(0, owners - 3)]
    pltpu.make_async_copy(sent, sent, row_send).wait()


def local(sizes, table, unique_ids, counts, inverse, lengths):
    nx, ny = sizes
    tables, rows_dev, width = table.shape
    owners = counts.shape[2]
    uniq = unique_ids.shape[2]
    cap = uniq // owners
    samples, _, depth = inverse.shape
    q_all = nx * CORES * ny
    slots = q_all * cap
    dims = (nx, ny, cap, rows_dev)
    vmem = pl.BlockSpec(memory_space=pltpu.VMEM)
    block = pltpu.VMEM((q_all, tables, cap, width), jnp.float32)
    far = pltpu.VMEM((q_all, cap, width), jnp.float32)
    out = pl.pallas_call(
        functools.partial(kernel, dims),
        out_shape=jax.ShapeDtypeStruct((samples * tables, width), jnp.float32),
        in_specs=[
            pl.BlockSpec(memory_space=pltpu.SMEM),
            vmem,
            vmem,
            vmem,
            pl.BlockSpec(memory_space=pl.ANY),
        ],
        out_specs=vmem,
        scratch_shapes=[
            pltpu.VMEM((tables * rows_dev, 1, width), jnp.float32),
            pltpu.SMEM((tables, owners), jnp.int32),
            pltpu.VMEM((owners, 1, 128), jnp.int32),
            pltpu.VMEM((owners, 1, 128), jnp.int32),
            pltpu.SMEM((owners, 1, 128), jnp.int32),
            pltpu.VMEM((tables, depth, samples), jnp.int32),
            [pltpu.VMEM((tables, depth, samples), jnp.int32)] * 2,
            pltpu.VMEM((3, tables, depth, samples), jnp.int32),
            pltpu.VMEM((3, tables, depth, samples), jnp.int32),
            pltpu.VMEM((16, slots, samples), jnp.bfloat16),
            pltpu.VMEM((owners, tables, cap, width), jnp.float32),
            [block] * 3 + [far] * 10,
            [pltpu.VMEM((width, samples), jnp.float32)] * (3 * tables),
            [pltpu.VMEM((width, samples), jnp.float32)] * (2 * tables),
            pltpu.SemaphoreType.REGULAR,
            pltpu.SemaphoreType.DMA,
            pltpu.SemaphoreType.DMA,
            pltpu.SemaphoreType.DMA((NZ,)),
            pltpu.SemaphoreType.DMA((NZ + 1,)),
            pltpu.SemaphoreType.DMA((2,)),
            pltpu.SemaphoreType.DMA((2,)),
            pltpu.SemaphoreType.DMA,
            pltpu.SemaphoreType.DMA((13,)),
            pltpu.SemaphoreType.DMA((2, 2)),
            pltpu.SemaphoreType.DMA((2, 2)),
        ],
        compiler_params=pltpu.CompilerParams(
            collective_id=0, has_side_effects=True, vmem_limit_bytes=56 << 20
        ),
        name="bags",
    )(
        counts[0],
        unique_ids.reshape(tables, uniq // 128, 128).transpose(1, 0, 2),
        inverse.transpose(1, 2, 0),
        lengths.T,
        table.reshape(tables * rows_dev, 1, width),
    )
    return out.reshape(samples, tables, width)


def solution(mesh):
    sizes = (mesh.shape["node"] // CORES, mesh.shape["chip"] // NZ)
    return jax.shard_map(
        functools.partial(local, sizes),
        mesh=mesh,
        in_specs=(
            P(None, ("node", "chip"), None),
            P(("node", "chip"), None, None),
            P(("node", "chip"), None, None),
            P(("node", "chip"), None, None),
            P(("node", "chip"), None),
        ),
        out_specs=P(("node", "chip"), None, None),
        check_vma=False,
    )
```

```python
import functools

import jax
import jax.numpy as jnp
from jax import lax
from jax.experimental import pallas as pl
from jax.experimental.pallas import tpu as pltpu
from jax.sharding import PartitionSpec as P

MESH = pl.DeviceIdType.MESH
NZ = 8
CORES = 2
FIELDS = 4
BITS = 8
CAP_BITS = 4
Z_BITS = 3

FAR = (
    ((5, -1, 1, 1), (4, -2, 1, 2), (3, 1, 2, 1), (6, 0, 1, 0), (2, 0, 2, 0)),
    ((4, 2, 2, 2), (3, 1, 2, 1), (5, -1, 1, 1), (2, 0, 2, 0), (6, 0, 1, 0)),
)
NEAR = ((1, 1, 0, 0), (7, -1, 0, 2), (0, 0, 0, 1))
ID_ORDER = (5, 4, 3, 6, 2, 1, 7, 0)


def near_slot(b):
    return b


def far_slot(t, g, b):
    at = [(route[2], route[3]) for route in FAR[t]].index((g, b))
    return len(NEAR) + t * len(FAR[0]) + at


def kernel(
    dims,
    counts,
    ids,
    inv,
    lens,
    table_hbm,
    out,
    table,
    start,
    msg,
    idbuf,
    idnum,
    code,
    code_in,
    group_of,
    unit_of,
    weight,
    send,
    recv,
    acc,
    part,
    ready,
    table_sem,
    id_send,
    id_recv,
    num_sem,
    code_send,
    code_recv,
    row_send,
    row_recv,
    part_send,
    part_recv,
):
    nx, ny, cap, rows_dev = dims
    q_all = nx * CORES * ny
    owners = q_all * NZ
    tables, depth, samples = inv.shape
    slots = q_all * cap
    words = slots // FIELDS
    node, chip = lax.axis_index("node"), lax.axis_index("chip")
    n_node, n_chip = nx * CORES, ny * NZ
    x, c, y, z = node // CORES, node % CORES, chip // NZ, chip % NZ
    mine = node * ny + y

    steps = [(dx, dc) for dx in range(nx) for dc in range(CORES)]
    node_to = [lax.rem(x + dx, nx) * CORES + lax.rem(c + dc, CORES) for dx, dc in steps]
    node_from = [
        lax.rem(x + nx - dx, nx) * CORES + lax.rem(c + CORES - dc, CORES) for dx, dc in steps
    ]

    def chip_at(dy, dz):
        return lax.rem(y + ny + dy, ny) * NZ + lax.rem(z + NZ + dz, NZ)

    def above(dz):
        return node, chip_at(0, dz)

    barrier = pltpu.get_barrier_semaphore()
    row = [(node, (chip + i) % n_chip) for i in range(1, n_chip)]
    column = [((node + i) % n_node, chip) for i in range(1, n_node)]
    for peer in row + column:
        pl.semaphore_signal(barrier, inc=1, device_id=peer, device_id_type=MESH)
    fetch = pltpu.make_async_copy(table_hbm, table, table_sem)
    fetch.start()

    lane = lax.broadcasted_iota(jnp.int32, (1, 128), 1)
    last = ids.shape[0] - 1

    def write_messages(n, sums):
        sums = list(sums)
        for u in range(8):
            o = n * 8 + u
            pieces = []
            for t in range(tables):
                at = sums[t]
                start[t, o] = at
                sums[t] = at + counts[t, o]
                r = jnp.minimum(at >> 7, last)
                l = at & 127
                a = ids[r, pl.ds(t, 1), :]
                b = ids[jnp.minimum(r + 1, last), pl.ds(t, 1), :]
                both = jnp.where(lane < l, b, a)
                pieces.append(pltpu.roll(both, (cap * t - l) & 127, 1))
            line = jnp.where(lane < cap, pieces[0], pieces[1])
            msg[o] = jnp.clip(line, 0, rows_dev - 1)
        return tuple(sums)

    lax.fori_loop(0, owners // 8, write_messages, (jnp.int32(0),) * tables)

    pl.semaphore_wait(barrier, n_chip + n_node - 2)
    for peer in column:
        pl.semaphore_signal(ready, inc=1, device_id=peer, device_id_type=MESH)
    pl.semaphore_wait(ready, n_node - 1)

    def send_ids(delta, dy, j):
        to = (node_from[j], chip_at(-dy, -delta))
        pltpu.make_async_remote_copy(
            msg.at[to[0] * n_chip + to[1]],
            idbuf[delta].at[dy * n_node + j],
            id_send,
            id_recv.at[delta],
            device_id=to,
            device_id_type=MESH,
        ).start()

    for delta in ID_ORDER:

        def one(dy, _, delta=delta):
            for j in range(n_node):
                if delta == 0 and j == 0:

                    @pl.when(dy > 0)
                    def _():
                        send_ids(delta, dy, j)
                else:
                    send_ids(delta, dy, j)
            return 0

        lax.fori_loop(0, ny, one, 0)

    position = lax.broadcasted_iota(jnp.int32, (depth, samples), 0)
    code_copies = {}
    for t in range(tables):
        index = inv[t]

        def shift(o, slot, t=t, index=index):
            n = counts[t, o]
            return slot + jnp.where(index >= start[t, o] + n, cap - n, 0)

        slot = lax.fori_loop(0, owners - 1, shift, index, unroll=5)
        plane = (slot >> CAP_BITS) & (NZ - 1)
        inside = (slot >> (CAP_BITS + Z_BITS)) * cap + (slot & (cap - 1))
        code[t][...] = jnp.where(position < lens[pl.ds(t, 1), :], plane * slots + inside, -1)
        for side, dz in ((0, 2), (1, -2)):
            copy = pltpu.make_async_remote_copy(
                code[t],
                code_in[tables * side + t],
                code_send.at[side, t],
                code_recv.at[side, t],
                device_id=above(dz),
                device_id_type=MESH,
            )
            copy.start()
            code_copies[side, t] = copy

    def split_codes(source, g, t):
        v = source[...]
        live = v >= 0
        inside = v & (slots - 1)
        group_of[g, t] = jnp.where(live, (v // slots) * words + (inside & (words - 1)), -1)
        unit_of[g, t] = jnp.where(live, 1 << (BITS * (inside // words)), 0)

    lanes = min(128, samples)
    rows_at = lax.broadcasted_iota(jnp.int32, (words, lanes), 0)

    def count(w, g, t, plane):
        wanted = rows_at + plane * words

        def tile(i, _):
            at = pl.multiple_of(i * lanes, lanes)

            def step(n, total):
                rows = pl.ds(pl.multiple_of(n * 8, 8), 8)
                groups = group_of.at[g, t, rows, pl.ds(at, lanes)]
                units = unit_of.at[g, t, rows, pl.ds(at, lanes)]
                for p in range(8):
                    hit = groups[pl.ds(p, 1), :] == wanted
                    total = total + jnp.where(hit, units[pl.ds(p, 1), :], 0)
                return total

            total = lax.fori_loop(0, depth // 8, step, jnp.zeros((words, lanes), jnp.int32))
            for f in range(FIELDS):
                part_count = (total >> (BITS * f)) & ((1 << BITS) - 1)
                weight[w, pl.ds(f * words, words), pl.ds(at, lanes)] = part_count.astype(
                    jnp.float32
                ).astype(jnp.bfloat16)
            return 0

        lax.fori_loop(0, samples // lanes, tile, 0)

    works = []
    for b in range(3):
        works += [(near_slot(b), 0, t, 2 * b + t, b - 1) for t in range(tables)]
    for t in range(tables):
        for _, _, g, b in FAR[t]:
            works.append((far_slot(t, g, b), g, t, len(works), b if g == 1 else -b))

    def count_all(g, t):
        for _, gg, tt, w, dz in works:
            if (gg, tt) == (g, t):
                count(w, g, t, lax.rem(z + NZ + dz, NZ))

    def ids_ready(delta):
        rows = pl.ds(0, q_all) if delta else pl.ds(1, q_all - 1)
        got = idbuf[delta].at[rows]
        pltpu.make_async_copy(got, got, id_recv.at[delta]).wait()
        copy = pltpu.make_async_copy(got, idnum[delta].at[rows], num_sem.at[delta])
        copy.start()
        return copy

    def collect(delta, i, t):
        k = delta * q_all + i
        for s in range(cap):
            r = idnum[delta][i, 0, t * cap + s]
            send[k, t, pl.ds(s, 1), :] = table[t * rows_dev + r]

    def serve(delta, dz, slot, t):
        def piece(k):
            return send.at[k] if t is None else send.at[k, t]

        def send_rows(k, dy, j):
            pltpu.make_async_remote_copy(
                piece(k),
                recv[slot].at[mine],
                row_send,
                row_recv.at[slot],
                device_id=(node_to[j], chip_at(dy, dz)),
                device_id_type=MESH,
            ).start()

        def line(dy, _):
            for j in range(n_node):
                k = delta * q_all + dy * n_node + j
                for tt in range(tables):
                    if t is None or t == tt:
                        collect(delta, dy * n_node + j, tt)
                if dz == 0 and j == 0:

                    @pl.when(dy > 0)
                    def _():
                        send_rows(k, dy, j)

                    @pl.when(dy == 0)
                    def _():
                        pltpu.make_async_copy(
                            piece(k), recv[slot].at[mine], row_recv.at[slot]
                        ).start()
                else:
                    send_rows(k, dy, j)
            return 0

        lax.fori_loop(0, ny, line, 0)

    def serve_far(t):
        for n, (delta, dz, g, b) in enumerate(FAR[t]):
            if t == 0:
                for ahead in ID_ORDER[n : n + 2] if n else ID_ORDER[:2]:
                    if ahead not in asked:
                        asked.add(ahead)
                        copies[ahead] = ids_ready(ahead)
                numbers_ready(delta)
            serve(delta, dz, far_slot(t, g, b), t)

    own_ids = pltpu.make_async_copy(
        msg.at[pl.ds(node * n_chip + chip, 1)], idnum[0].at[pl.ds(0, 1)], num_sem.at[NZ]
    )
    own_ids.start()
    copies = {}
    asked = set()

    def numbers_ready(delta):
        if delta in copies:
            copies.pop(delta).wait()

    fetch.wait()

    def rows_ready(slot):
        got = recv[slot]
        pltpu.make_async_copy(got, got, row_recv.at[slot]).wait()

    def pool(slot, g, t, w, first):
        rows = recv[slot][:, t] if g == 0 else recv[slot][...]
        rows = rows.reshape(slots, 128).T
        high = rows.astype(jnp.bfloat16)
        low = (rows - high.astype(jnp.float32)).astype(jnp.bfloat16)
        both = jnp.dot(
            jnp.concatenate([high, low], axis=0), weight[w], preferred_element_type=jnp.float32
        )
        new = both[:128] + both[128:]
        total = acc[tables * g + t]
        total[...] = new if first else total[...] + new

    part_copies = []

    def pool_far(t):
        for g in ((1, 2), (2, 1))[t]:
            mine_now = [work for work in works if work[1:3] == (g, t)]
            for n, (slot, _, _, w, _) in enumerate(mine_now):
                rows_ready(slot)
                pool(slot, g, t, w, n == 0)
            copy = pltpu.make_async_remote_copy(
                acc[tables * g + t],
                part[tables * (g - 1) + t],
                part_send.at[g - 1, t],
                part_recv.at[g - 1, t],
                device_id=above(-2 if g == 1 else 2),
                device_id_type=MESH,
            )
            copy.start()
            part_copies.append((t, copy))

    for t in range(tables):
        serve_far(t)
        for g in ((1, 2), (2, 1))[t]:
            code_copies[g - 1, t].wait_recv()
            split_codes(code_in[tables * (g - 1) + t], g, t)
            count_all(g, t)
    pool_far(0)
    for delta in ID_ORDER[5:]:
        if delta not in asked:
            copies[delta] = ids_ready(delta)
    own_ids.wait()
    for delta in ID_ORDER[5:]:
        numbers_ready(delta)
    for delta, dz, _, b in NEAR:
        serve(delta, dz, near_slot(b), None)
    for t in range(tables):
        split_codes(code[t], 0, t)
        count_all(0, t)
    pool_far(1)

    for n, b in enumerate((1, 0, 2)):
        rows_ready(near_slot(b))
        for slot, g, t, w, _ in works:
            if g == 0 and slot == near_slot(b):
                pool(slot, g, t, w, n == 0)
    for t in range(tables):
        for tt, copy in part_copies:
            if tt == t:
                copy.wait_recv()
        out[pl.ds(t, samples, stride=tables), :] = (
            acc[t][...] + (part[t][...] + part[tables + t][...])
        ).T

    for copy in code_copies.values():
        copy.wait_send()
    for _, copy in part_copies:
        copy.wait_send()
    pltpu.make_async_copy(msg.at[pl.ds(1, owners - 1)], msg.at[pl.ds(1, owners - 1)], id_send).wait()
    sent = send.at[pl.ds(0, owners - 3)]
    pltpu.make_async_copy(sent, sent, row_send).wait()


def local(sizes, table, unique_ids, counts, inverse, lengths):
    nx, ny = sizes
    tables, rows_dev, width = table.shape
    owners = counts.shape[2]
    uniq = unique_ids.shape[2]
    cap = uniq // owners
    samples, _, depth = inverse.shape
    q_all = nx * CORES * ny
    slots = q_all * cap
    dims = (nx, ny, cap, rows_dev)
    vmem = pl.BlockSpec(memory_space=pltpu.VMEM)
    block = pltpu.VMEM((q_all, tables, cap, width), jnp.float32)
    far = pltpu.VMEM((q_all, cap, width), jnp.float32)
    out = pl.pallas_call(
        functools.partial(kernel, dims),
        out_shape=pltpu.VMEM((samples * tables, width), jnp.float32),
        in_specs=[
            pl.BlockSpec(memory_space=pltpu.SMEM),
            vmem,
            vmem,
            vmem,
            pl.BlockSpec(memory_space=pl.ANY),
        ],
        out_specs=vmem,
        scratch_shapes=[
            pltpu.VMEM((tables * rows_dev, 1, width), jnp.float32),
            pltpu.SMEM((tables, owners), jnp.int32),
            pltpu.VMEM((owners, 1, 128), jnp.int32),
            [pltpu.VMEM((q_all, 1, 128), jnp.int32)] * NZ,
            [pltpu.SMEM((q_all, 1, 128), jnp.int32)] * NZ,
            [pltpu.VMEM((depth, samples), jnp.int32)] * tables,
            [pltpu.VMEM((depth, samples), jnp.int32)] * (2 * tables),
            pltpu.VMEM((3, tables, depth, samples), jnp.int32),
            pltpu.VMEM((3, tables, depth, samples), jnp.int32),
            pltpu.VMEM((16, slots, samples), jnp.bfloat16),
            pltpu.VMEM((owners, tables, cap, width), jnp.float32),
            [block] * 3 + [far] * 10,
            [pltpu.VMEM((width, samples), jnp.float32)] * (3 * tables),
            [pltpu.VMEM((width, samples), jnp.float32)] * (2 * tables),
            pltpu.SemaphoreType.REGULAR,
            pltpu.SemaphoreType.DMA,
            pltpu.SemaphoreType.DMA,
            pltpu.SemaphoreType.DMA((NZ,)),
            pltpu.SemaphoreType.DMA((NZ + 1,)),
            pltpu.SemaphoreType.DMA((2, 2)),
            pltpu.SemaphoreType.DMA((2, 2)),
            pltpu.SemaphoreType.DMA,
            pltpu.SemaphoreType.DMA((13,)),
            pltpu.SemaphoreType.DMA((2, 2)),
            pltpu.SemaphoreType.DMA((2, 2)),
        ],
        compiler_params=pltpu.CompilerParams(
            collective_id=0, has_side_effects=True, vmem_limit_bytes=56 << 20
        ),
        name="bags",
    )(
        counts[0],
        unique_ids.reshape(tables, uniq // 128, 128).transpose(1, 0, 2),
        inverse.transpose(1, 2, 0),
        lengths.T,
        table.reshape(tables * rows_dev, 1, width),
    )
    return out.reshape(samples, tables, width)


def solution(mesh):
    sizes = (mesh.shape["node"] // CORES, mesh.shape["chip"] // NZ)
    return jax.shard_map(
        functools.partial(local, sizes),
        mesh=mesh,
        in_specs=(
            P(None, ("node", "chip"), None),
            P(("node", "chip"), None, None),
            P(("node", "chip"), None, None),
            P(("node", "chip"), None, None),
            P(("node", "chip"), None),
        ),
        out_specs=P(("node", "chip"), None, None),
        check_vma=False,
    )
```

```python
import functools

import jax
import jax.numpy as jnp
from jax import lax
from jax.experimental import pallas as pl
from jax.experimental.pallas import tpu as pltpu
from jax.sharding import PartitionSpec as P

MESH = pl.DeviceIdType.MESH
NZ = 8
CORES = 2
FIELDS = 4
BITS = 8
CAP_BITS = 4
Z_BITS = 3

FAR = (
    ((5, -1, 1, 1), (4, -2, 1, 2), (3, 1, 2, 1), (6, 0, 1, 0), (2, 0, 2, 0)),
    ((4, 2, 2, 2), (3, 1, 2, 1), (5, -1, 1, 1), (2, 0, 2, 0), (6, 0, 1, 0)),
)
NEAR = (
    (1, 3, 0, 0, 7, 0),
    (2, 4, 0, 0, 1, 0),
    (3, 0, 1, -1, 1, 1),
    (4, 0, 1, 1, 7, -1),
    (0, 0, 0, 0, 0, 0),
    (5, 0, 1, 0, 0, 0),
)
ID_ORDER = (5, 4, 3, 6, 2, 1, 7, 0)


def far_slot(t, g, b):
    at = [(route[2], route[3]) for route in FAR[t]].index((g, b))
    return len(NEAR) + t * len(FAR[0]) + at


def kernel(
    dims,
    counts,
    ids,
    inv,
    lens,
    table_hbm,
    out,
    table,
    start,
    msg,
    idbuf,
    idnum,
    code,
    code_in,
    group_of,
    unit_of,
    weight,
    send,
    recv,
    acc,
    part,
    inbox,
    ready,
    table_sem,
    id_send,
    id_recv,
    num_sem,
    code_send,
    code_recv,
    row_send,
    row_recv,
    part_send,
    part_recv,
    inbox_send,
    inbox_recv,
):
    nx, ny, cap, rows_dev = dims
    q_all = nx * CORES * ny
    owners = q_all * NZ
    tables, depth, samples = inv.shape
    slots = q_all * cap
    words = slots // FIELDS
    node, chip = lax.axis_index("node"), lax.axis_index("chip")
    n_node, n_chip = nx * CORES, ny * NZ
    x, c, y, z = node // CORES, node % CORES, chip // NZ, chip % NZ
    mine = node * ny + y

    steps = [(dx, dc) for dx in range(nx) for dc in range(CORES)]
    node_to = [lax.rem(x + dx, nx) * CORES + lax.rem(c + dc, CORES) for dx, dc in steps]
    node_from = [
        lax.rem(x + nx - dx, nx) * CORES + lax.rem(c + CORES - dc, CORES) for dx, dc in steps
    ]

    def chip_at(dy, dz):
        return lax.rem(y + ny + dy, ny) * NZ + lax.rem(z + NZ + dz, NZ)

    def above(dz):
        return node, chip_at(0, dz)

    barrier = pltpu.get_barrier_semaphore()
    row = [(node, (chip + i) % n_chip) for i in range(1, n_chip)]
    column = [((node + i) % n_node, chip) for i in range(1, n_node)]
    for peer in row + column:
        pl.semaphore_signal(barrier, inc=1, device_id=peer, device_id_type=MESH)
    fetch = pltpu.make_async_copy(table_hbm, table, table_sem)
    fetch.start()

    lane = lax.broadcasted_iota(jnp.int32, (1, 128), 1)
    last = ids.shape[0] - 1

    def write_messages(n, sums):
        sums = list(sums)
        for u in range(8):
            o = n * 8 + u
            pieces = []
            for t in range(tables):
                at = sums[t]
                start[t, o] = at
                sums[t] = at + counts[t, o]
                r = jnp.minimum(at >> 7, last)
                l = at & 127
                a = ids[r, pl.ds(t, 1), :]
                b = ids[jnp.minimum(r + 1, last), pl.ds(t, 1), :]
                both = jnp.where(lane < l, b, a)
                pieces.append(pltpu.roll(both, (cap * t - l) & 127, 1))
            line = jnp.where(lane < cap, pieces[0], pieces[1])
            msg[o] = jnp.clip(line, 0, rows_dev - 1)
        return tuple(sums)

    lax.fori_loop(0, owners // 8, write_messages, (jnp.int32(0),) * tables)

    pl.semaphore_wait(barrier, n_chip + n_node - 2)
    for peer in column:
        pl.semaphore_signal(ready, inc=1, device_id=peer, device_id_type=MESH)
    pl.semaphore_wait(ready, n_node - 1)

    def send_ids(delta, dy, j):
        to = (node_from[j], chip_at(-dy, -delta))
        pltpu.make_async_remote_copy(
            msg.at[to[0] * n_chip + to[1]],
            idbuf[delta].at[dy * n_node + j],
            id_send,
            id_recv.at[delta],
            device_id=to,
            device_id_type=MESH,
        ).start()

    for delta in ID_ORDER:

        def one(dy, _, delta=delta):
            for j in range(n_node):
                if delta == 0 and j == 0:

                    @pl.when(dy > 0)
                    def _():
                        send_ids(delta, dy, j)
                else:
                    send_ids(delta, dy, j)
            return 0

        lax.fori_loop(0, ny, one, 0)

    position = lax.broadcasted_iota(jnp.int32, (depth, samples), 0)
    code_copies = {}
    for t in range(tables):
        index = inv[t]

        def shift(o, slot, t=t, index=index):
            n = counts[t, o]
            return slot + jnp.where(index >= start[t, o] + n, cap - n, 0)

        slot = lax.fori_loop(0, owners - 1, shift, index, unroll=5)
        plane = (slot >> CAP_BITS) & (NZ - 1)
        inside = (slot >> (CAP_BITS + Z_BITS)) * cap + (slot & (cap - 1))
        code[t][...] = jnp.where(position < lens[pl.ds(t, 1), :], plane * slots + inside, -1)
        for side, dz in ((0, 2), (1, -2), (2, 1), (3, -1))[: 2 if t else 4]:
            copy = pltpu.make_async_remote_copy(
                code[t],
                code_in[2 * side + t if side < 2 else side + 2],
                code_send.at[side, t],
                code_recv.at[side, t],
                device_id=above(dz),
                device_id_type=MESH,
            )
            copy.start()
            code_copies[side, t] = copy

    def split_codes(source, g, t):
        v = source[...]
        live = v >= 0
        inside = v & (slots - 1)
        group_of[g, t] = jnp.where(live, (v // slots) * words + (inside & (words - 1)), -1)
        unit_of[g, t] = jnp.where(live, 1 << (BITS * (inside // words)), 0)

    lanes = min(128, samples)
    rows_at = lax.broadcasted_iota(jnp.int32, (words, lanes), 0)

    def count(w, g, t, plane):
        wanted = rows_at + plane * words

        def tile(i, _):
            at = pl.multiple_of(i * lanes, lanes)

            def step(n, total):
                rows = pl.ds(pl.multiple_of(n * 8, 8), 8)
                groups = group_of.at[g, t, rows, pl.ds(at, lanes)]
                units = unit_of.at[g, t, rows, pl.ds(at, lanes)]
                for p in range(8):
                    hit = groups[pl.ds(p, 1), :] == wanted
                    total = total + jnp.where(hit, units[pl.ds(p, 1), :], 0)
                return total

            total = lax.fori_loop(0, depth // 8, step, jnp.zeros((words, lanes), jnp.int32))
            for f in range(FIELDS):
                part_count = (total >> (BITS * f)) & ((1 << BITS) - 1)
                weight[w, pl.ds(f * words, words), pl.ds(at, lanes)] = part_count.astype(
                    jnp.float32
                ).astype(jnp.bfloat16)
            return 0

        lax.fori_loop(0, samples // lanes, tile, 0)

    works = [(slot, g, t, n, dz) for n, (slot, g, t, dz, _, _) in enumerate(NEAR)]
    for t in range(tables):
        for _, _, g, b in FAR[t]:
            works.append((far_slot(t, g, b), g, t, len(works), b if g == 1 else -b))

    def count_all(g, t):
        for _, gg, tt, w, dz in works:
            if (gg, tt) == (g, t):
                count(w, g, t, lax.rem(z + NZ + dz, NZ))

    def ids_ready(delta):
        rows = pl.ds(0, q_all) if delta else pl.ds(1, q_all - 1)
        got = idbuf[delta].at[rows]
        pltpu.make_async_copy(got, got, id_recv.at[delta]).wait()
        copy = pltpu.make_async_copy(got, idnum[delta].at[rows], num_sem.at[delta])
        copy.start()
        return copy

    def collect(delta, i, t):
        k = delta * q_all + i
        for s in range(cap):
            r = idnum[delta][i, 0, t * cap + s]
            send[k, t, pl.ds(s, 1), :] = table[t * rows_dev + r]

    def serve(delta, dz, slot, t):
        def piece(k):
            return send.at[k, t]

        def send_rows(k, dy, j):
            pltpu.make_async_remote_copy(
                piece(k),
                recv[slot].at[mine],
                row_send,
                row_recv.at[slot],
                device_id=(node_to[j], chip_at(dy, dz)),
                device_id_type=MESH,
            ).start()

        def line(dy, _):
            for j in range(n_node):
                k = delta * q_all + dy * n_node + j
                collect(delta, dy * n_node + j, t)
                if dz == 0 and j == 0:

                    @pl.when(dy > 0)
                    def _():
                        send_rows(k, dy, j)

                    @pl.when(dy == 0)
                    def _():
                        pltpu.make_async_copy(
                            piece(k), recv[slot].at[mine], row_recv.at[slot]
                        ).start()
                else:
                    send_rows(k, dy, j)
            return 0

        lax.fori_loop(0, ny, line, 0)

    def serve_far(t):
        for n, (delta, dz, g, b) in enumerate(FAR[t]):
            if t == 0:
                for ahead in ID_ORDER[n : n + 2] if n else ID_ORDER[:2]:
                    if ahead not in asked:
                        asked.add(ahead)
                        copies[ahead] = ids_ready(ahead)
                numbers_ready(delta)
            serve(delta, dz, far_slot(t, g, b), t)

    own_ids = pltpu.make_async_copy(
        msg.at[pl.ds(node * n_chip + chip, 1)], idnum[0].at[pl.ds(0, 1)], num_sem.at[NZ]
    )
    own_ids.start()
    copies = {}
    asked = set()

    def numbers_ready(delta):
        if delta in copies:
            copies.pop(delta).wait()

    fetch.wait()

    def rows_ready(slot):
        got = recv[slot]
        pltpu.make_async_copy(got, got, row_recv.at[slot]).wait()

    def acc_at(g, t):
        return 2 * g + t if g < 3 else g + 3

    def pool(slot, g, t, w, first):
        rows = recv[slot][...]
        rows = rows.reshape(slots, 128).T
        high = rows.astype(jnp.bfloat16)
        low = (rows - high.astype(jnp.float32)).astype(jnp.bfloat16)
        both = jnp.dot(
            jnp.concatenate([high, low], axis=0), weight[w], preferred_element_type=jnp.float32
        )
        new = both[:128] + both[128:]
        total = acc[acc_at(g, t)]
        total[...] = new if first else total[...] + new

    part_copies = []
    inbox_copies = []

    def pool_far(t):
        for g in ((1, 2), (2, 1))[t]:
            mine_now = [work for work in works if work[1:3] == (g, t)]
            for n, (slot, _, _, w, _) in enumerate(mine_now):
                rows_ready(slot)
                pool(slot, g, t, w, n == 0)
            if t == 0:
                copy = pltpu.make_async_remote_copy(
                    acc[2 * g],
                    inbox[g - 1],
                    inbox_send.at[g - 1],
                    inbox_recv.at[g - 1],
                    device_id=above(-1 if g == 1 else 1),
                    device_id_type=MESH,
                )
                copy.start()
                inbox_copies.append(copy)
            else:
                send_part(acc[2 * g + 1], g - 1, t, -2 if g == 1 else 2)

    def send_part(total, side, t, dz):
        copy = pltpu.make_async_remote_copy(
            total,
            part[2 * side + t],
            part_send.at[side, t],
            part_recv.at[side, t],
            device_id=above(dz),
            device_id_type=MESH,
        )
        copy.start()
        part_copies.append((t, copy))

    def pool_next(g):
        slot, _, t, w, _ = [work for work in works if work[1] == g][0]
        rows_ready(slot)
        pool(slot, g, t, w, True)
        inbox_copies[g - 3].wait_recv()
        total = acc[acc_at(g, t)]
        total[...] = total[...] + inbox[g - 3][...]
        send_part(total, g - 3, 0, -1 if g == 3 else 1)

    for t in range(tables):
        serve_far(t)
        for g in ((1, 2), (2, 1))[t]:
            code_copies[g - 1, t].wait_recv()
            split_codes(code_in[2 * (g - 1) + t], g, t)
            count_all(g, t)
    pool_far(0)
    for delta in ID_ORDER[5:]:
        if delta not in asked:
            copies[delta] = ids_ready(delta)
    own_ids.wait()
    for delta in ID_ORDER[5:]:
        numbers_ready(delta)
    for slot, _, t, _, delta, dz in NEAR:
        serve(delta, dz, slot, t)
    for g in (3, 4):
        code_copies[g - 1, 0].wait_recv()
        split_codes(code_in[g + 1], g, 0)
        count_all(g, 0)
    for t in range(tables):
        split_codes(code[t], 0, t)
        count_all(0, t)
    pool_far(1)
    pool_next(3)
    pool_next(4)

    done = set()
    for slot, g, t, w, _ in works[: len(NEAR)]:
        if g == 0:
            rows_ready(slot)
            pool(slot, g, t, w, t not in done)
            done.add(t)
    for t in range(tables):
        for tt, copy in part_copies:
            if tt == t:
                copy.wait_recv()
        out[pl.ds(t, samples, stride=tables), :] = (
            acc[t][...] + (part[t][...] + part[tables + t][...])
        ).T

    for copy in code_copies.values():
        copy.wait_send()
    for _, copy in part_copies:
        copy.wait_send()
    for copy in inbox_copies:
        copy.wait_send()
    pltpu.make_async_copy(msg.at[pl.ds(1, owners - 1)], msg.at[pl.ds(1, owners - 1)], id_send).wait()
    sent = send.at[pl.ds(0, owners - 4)]
    pltpu.make_async_copy(sent, sent, row_send).wait()


def local(sizes, table, unique_ids, counts, inverse, lengths):
    nx, ny = sizes
    tables, rows_dev, width = table.shape
    owners = counts.shape[2]
    uniq = unique_ids.shape[2]
    cap = uniq // owners
    samples, _, depth = inverse.shape
    q_all = nx * CORES * ny
    slots = q_all * cap
    dims = (nx, ny, cap, rows_dev)
    vmem = pl.BlockSpec(memory_space=pltpu.VMEM)
    far = pltpu.VMEM((q_all, cap, width), jnp.float32)
    out = pl.pallas_call(
        functools.partial(kernel, dims),
        out_shape=pltpu.VMEM((samples * tables, width), jnp.float32),
        in_specs=[
            pl.BlockSpec(memory_space=pltpu.SMEM),
            vmem,
            vmem,
            vmem,
            pl.BlockSpec(memory_space=pl.ANY),
        ],
        out_specs=vmem,
        scratch_shapes=[
            pltpu.VMEM((tables * rows_dev, 1, width), jnp.float32),
            pltpu.SMEM((tables, owners), jnp.int32),
            pltpu.VMEM((owners, 1, 128), jnp.int32),
            [pltpu.VMEM((q_all, 1, 128), jnp.int32)] * NZ,
            [pltpu.SMEM((q_all, 1, 128), jnp.int32)] * NZ,
            [pltpu.VMEM((depth, samples), jnp.int32)] * tables,
            [pltpu.VMEM((depth, samples), jnp.int32)] * 6,
            pltpu.VMEM((5, tables, depth, samples), jnp.int32),
            pltpu.VMEM((5, tables, depth, samples), jnp.int32),
            pltpu.VMEM((16, slots, samples), jnp.bfloat16),
            pltpu.VMEM((owners, tables, cap, width), jnp.float32),
            [far] * 16,
            [pltpu.VMEM((width, samples), jnp.float32)] * 8,
            [pltpu.VMEM((width, samples), jnp.float32)] * (2 * tables),
            [pltpu.VMEM((width, samples), jnp.float32)] * 2,
            pltpu.SemaphoreType.REGULAR,
            pltpu.SemaphoreType.DMA,
            pltpu.SemaphoreType.DMA,
            pltpu.SemaphoreType.DMA((NZ,)),
            pltpu.SemaphoreType.DMA((NZ + 1,)),
            pltpu.SemaphoreType.DMA((4, 2)),
            pltpu.SemaphoreType.DMA((4, 2)),
            pltpu.SemaphoreType.DMA,
            pltpu.SemaphoreType.DMA((16,)),
            pltpu.SemaphoreType.DMA((2, 2)),
            pltpu.SemaphoreType.DMA((2, 2)),
            pltpu.SemaphoreType.DMA((2,)),
            pltpu.SemaphoreType.DMA((2,)),
        ],
        compiler_params=pltpu.CompilerParams(
            collective_id=0, has_side_effects=True, vmem_limit_bytes=56 << 20
        ),
        name="bags",
    )(
        counts[0],
        unique_ids.reshape(tables, uniq // 128, 128).transpose(1, 0, 2),
        inverse.transpose(1, 2, 0),
        lengths.T,
        table.reshape(tables * rows_dev, 1, width),
    )
    return out.reshape(samples, tables, width)


def solution(mesh):
    sizes = (mesh.shape["node"] // CORES, mesh.shape["chip"] // NZ)
    return jax.shard_map(
        functools.partial(local, sizes),
        mesh=mesh,
        in_specs=(
            P(None, ("node", "chip"), None),
            P(("node", "chip"), None, None),
            P(("node", "chip"), None, None),
            P(("node", "chip"), None, None),
            P(("node", "chip"), None),
        ),
        out_specs=P(("node", "chip"), None, None),
        check_vma=False,
    )
```
